256 devices in a mesh: lb: 8 (over z), rb: 16 (over x, y), wa: 2 (over core).
Axes of the slice: x: 4, y: 4, z: 8, core: 2. Of those that a mesh axis runs over, the one named last changes fastest.
Arguments:
- initial_guess: bfloat16 [8192, 4, 128], P(('lb', 'rb')), may hold values from -6 to 6
- left_environment: bfloat16 [8, 8, 16, 64, 8192], P('wa', None, 'rb', None, 'lb'), may hold values from -12 to 12, as said below
- right_environment: bfloat16 [128, 8, 128], replicated, may hold values from -12 to 12, as said below
- operator_blocks: float32 [16, 4, 4], replicated, may hold values from -4 to 4
- operator_pairs: int32 [16, 2], replicated, may hold values from 0 to 7
Outputs:
- ritz_vector: float32 [8192, 4, 128], P(('lb', 'rb'))
- residual: float32 [8192, 4, 128], P(('lb', 'rb'))
The draws below stay inside these ranges and needn't reach their ends.
Inputs may be any that keep to these rules, and one draw needn't show every extreme that they name: `operator_pairs`: each row names the left and the right MPO index of one operator block; blocks with the same pair add. `left_environment`: for each MPO index the [8192, 8192] matrix is symmetric. `right_environment`: for each MPO index the matrix over the two right bond states is symmetric.
All inputs are finite; a program needn't handle non-finite values.
Results may differ from the reference program's by a relative error of at most 0.014.
Values may be sent and summed in bfloat16 or wider, within the bound.
No kernel may reach another device: no remote copies, remote signals or barrier semaphores. Data moves between devices by JAX's collectives and lax.ppermute only.
A program may use at most 128 MiB of HBM per device.

```python
import jax
import jax.numpy as jnp
from jax import lax

DL = 8192
RB = 128
W = 8
NB = 16
ITERS = 3
SWEEPS = 8
S = 4
N_LB = 8
N_RB = 16


def draw_left_environment(key, part):
    noise_key = jax.random.fold_in(key, 11)
    scale_key = jax.random.fold_in(key, 12)
    noise = jax.random.normal(noise_key, (W, DL, DL), jnp.float32)
    symmetric = (noise + jnp.swapaxes(noise, 1, 2)) * (0.5 / jnp.sqrt(DL * 1.0))
    scales = jnp.exp(jax.random.uniform(scale_key, (W, DL), jnp.float32, 0.0, 2.0))
    positions = jnp.arange(DL, dtype=jnp.int32)
    symmetric = symmetric.at[:, positions, positions].add(scales)
    return symmetric.reshape(W, N_LB, N_RB, DL // (N_LB * N_RB), DL).astype(jnp.bfloat16)


def draw_right_environment(key, part):
    noise_key = jax.random.fold_in(key, 21)
    scale_key = jax.random.fold_in(key, 22)
    noise = jax.random.normal(noise_key, (RB, W, RB), jnp.float32)
    symmetric = (noise + jnp.transpose(noise, (2, 1, 0))) * (0.5 / jnp.sqrt(RB * 1.0))
    scales = jnp.exp(jax.random.uniform(scale_key, (W, RB), jnp.float32, 0.0, 2.0))
    symmetric = symmetric + jnp.eye(RB, dtype=jnp.float32)[:, None, :] * scales[None, :, :]
    return symmetric.astype(jnp.bfloat16)


def place_ends(entries, rng, least, top_value):
    shape = entries.shape
    place = [jax.random.randint(jax.random.fold_in(rng, axis), (), 0, shape[axis]) for axis in range(len(shape))]
    entries = entries.at[tuple(place)].set(least)
    longest = shape.index(max(shape))
    place[longest] = (place[longest] + 1) % shape[longest]
    return entries.at[tuple(place)].set(top_value)


def block_scale(key, dims, split, smallest, high):
    loudness, own = 1.0, jax.random.fold_in(key, 6)
    for axis_at, parts in split:
        draws = jnp.exp(jax.random.uniform(jax.random.fold_in(own, axis_at), (parts,), jnp.float32, smallest / len(split), high / len(split)))
        loudness = loudness * jnp.repeat(draws, dims[axis_at] // parts).reshape([-1 if axis == axis_at else 1 for axis in range(len(dims))])
    return loudness


def scatter_about(key, extent, deviation, reach, shards=(), kind=jnp.bfloat16):
    values = deviation * jax.random.normal(key, extent, jnp.float32)
    if shards:
        values = values * block_scale(key, extent, shards, -0.22, 0.18)
    return jnp.clip(values, -reach, reach).astype(kind)


def setup_inputs(seed: int = 0) -> dict:
    key_list = jax.random.split(jax.random.key(seed), 6)
    initial_guess = scatter_about(key_list[0], (DL, S, RB), 1.0, 6.0, ((0, 128),))
    left_environment = draw_left_environment(jax.random.fold_in(key_list[5], 71), 0)
    right_environment = draw_right_environment(jax.random.fold_in(key_list[5], 71), 0)
    operator_blocks = scatter_about(key_list[3], (NB, S, S), 0.3, 4.0, (), jnp.float32)
    operator_pairs = place_ends(jax.random.randint(key_list[4], (NB, 2), 0, W), jax.random.fold_in(key_list[4], 1), 0, W - 1).astype(jnp.int32)
    return dict(initial_guess=initial_guess, left_environment=left_environment, right_environment=right_environment, operator_blocks=operator_blocks, operator_pairs=operator_pairs)


highest = lax.Precision.HIGHEST
epsilon = 1e-06

def lowest_pair(matrix):
    matrix_order = matrix.shape[0]
    vectors = jnp.eye(matrix_order, dtype=jnp.float32)
    for rounds in range(SWEEPS):
        for first_row in range(matrix_order):
            for second_row in range(first_row + 1, matrix_order):
                rotation_angle = 0.5 * jnp.arctan2(2.0 * matrix[first_row, second_row], matrix[second_row, second_row] - matrix[first_row, first_row])
                cosine = jnp.cos(rotation_angle)
                sine_value = jnp.sin(rotation_angle)
                rotation = jnp.eye(matrix_order, dtype=jnp.float32)
                rotation = rotation.at[first_row, first_row].set(cosine).at[second_row, second_row].set(cosine)
                rotation = rotation.at[first_row, second_row].set(sine_value).at[second_row, first_row].set(-sine_value)
                matrix = jnp.dot(rotation.T, jnp.dot(matrix, rotation, precision=highest), precision=highest)
                vectors = jnp.dot(vectors, rotation, precision=highest)
    values = jnp.diagonal(matrix)
    chosen = (jnp.arange(matrix_order, dtype=jnp.int32) == jnp.argmin(values).astype(jnp.int32)).astype(jnp.float32)
    ritz_value = jnp.sum(values * chosen)
    weights = jnp.dot(vectors, chosen, precision=highest)
    weights = jnp.where(weights[0] < 0.0, -weights, weights)
    return (ritz_value, weights)

def dense_operator(operator_blocks, operator_pairs, levels):
    symmetric = 0.5 * (operator_blocks + jnp.swapaxes(operator_blocks, 1, 2))
    indices = jnp.arange(levels, dtype=jnp.int32)
    left_hot = (operator_pairs[:, 0:1] == indices[None, :]).astype(jnp.float32)
    right_hot = (operator_pairs[:, 1:2] == indices[None, :]).astype(jnp.float32)
    return jnp.einsum('nw,nv,nts->wvts', left_hot, right_hot, symmetric, precision=highest)

def contract_right(vector_rows, right_matrix, local_operator):
    row_count, physical, window = vector_rows.shape
    levels = local_operator.shape[1]
    mixed = jnp.dot(vector_rows.reshape(row_count * physical, window), right_matrix, preferred_element_type=jnp.float32)
    mixed = mixed.reshape(row_count, physical, levels, window)
    return jnp.einsum('kvts,nsvb->kntb', local_operator, mixed, precision=highest).astype(jnp.bfloat16)

def combine(members, weights):
    total = weights[0] * members[0]
    for member_index in range(1, len(members)):
        total = total + weights[member_index] * members[member_index]
    return total

def reference(initial_guess, left_environment, right_environment, operator_blocks, operator_pairs):
    total_count = DL * S * RB
    left_matrix = left_environment.reshape(W, DL, DL)
    right_matrix = right_environment.reshape(RB, W * RB)
    operator = dense_operator(operator_blocks, operator_pairs, W)

    def apply_hamiltonian(vector):
        inner_terms = contract_right(vector.astype(jnp.bfloat16), right_matrix, operator)
        flat = inner_terms.reshape(W, DL, S * RB)
        image = jnp.zeros((DL, S * RB), jnp.float32)
        for level in range(W):
            image = image + jnp.dot(left_matrix[level], flat[level], preferred_element_type=jnp.float32)
        return image.reshape(DL, S, RB)

    def mean_product(first_array, second_array):
        return jnp.sum(first_array * second_array) / total_count
    left_diag = jnp.diagonal(left_matrix, axis1=1, axis2=2).astype(jnp.float32)
    operator_diag = jnp.diagonal(operator, axis1=2, axis2=3)
    right_diag = jnp.diagonal(right_environment, axis1=0, axis2=2).astype(jnp.float32)
    diagonal_values = jnp.einsum('ka,kvs,vb->asb', left_diag, operator_diag, right_diag, precision=highest)
    start_vector = initial_guess.astype(jnp.float32)
    basis = [start_vector * lax.rsqrt(mean_product(start_vector, start_vector) + epsilon)]
    images = [apply_hamiltonian(basis[0])]
    subspace = jnp.zeros((ITERS + 1, ITERS + 1), jnp.float32)
    subspace = subspace.at[0, 0].set(mean_product(basis[0], images[0]))
    for step_index in range(ITERS):
        filled = step_index + 1
        ritz_value, weights = lowest_pair(subspace[:filled, :filled])
        ritz_now = combine(basis, weights)
        residual_now = combine(images, weights) - ritz_value * ritz_now
        correction = residual_now / (jnp.abs(diagonal_values - ritz_value) + 1.0)
        correlations = jnp.stack([mean_product(member, correction) for member in basis])
        correction = correction - combine(basis, correlations)
        new_vector = correction * lax.rsqrt(mean_product(correction, correction) + epsilon)
        new_image = apply_hamiltonian(new_vector)
        basis.append(new_vector)
        images.append(new_image)
        row_values = jnp.stack([mean_product(member, new_image) for member in basis])
        subspace = subspace.at[filled, :filled + 1].set(row_values).at[:filled + 1, filled].set(row_values)
    ritz_value, weights = lowest_pair(subspace)
    ritz_vector = combine(basis, weights)
    residual = combine(images, weights) - ritz_value * ritz_vector
    return (ritz_vector, residual)
```

```python
import functools

import jax
import jax.numpy as jnp
from jax import lax
from jax.experimental import pallas as pl
from jax.experimental.pallas import tpu as pltpu
from jax.sharding import Mesh
from jax.sharding import PartitionSpec as P

ITERS = 3
SWEEPS = 8
S = 4
LANES = 128
HALF = 32
TILE = S * HALF
EXT = 16
N_LB = 8
N_RB = 16
RB = ("rb_0", "rb_1")
LB_RB = ("lb", "rb_0", "rb_1")
LB_WA = ("lb", "wa")
RB_WA = ("rb_0", "rb_1", "wa")
SEGMENTS = ((0, N_RB, 0), (N_RB, N_RB, 1), (2 * N_RB, N_LB, 0), (2 * N_RB + N_LB, N_LB, 1))
BLOCKS = 2 * (N_RB + N_LB)

highest = lax.Precision.HIGHEST
epsilon = 1e-06
f32 = jnp.float32
bf16 = jnp.bfloat16


def rotate(matrix, vectors, order, p, q):
    y = 2.0 * matrix[p, q]
    x = matrix[q, q] - matrix[p, p]
    large = jnp.maximum(jnp.abs(x), jnp.abs(y))
    zero = large == 0.0
    scale = 1.0 / jnp.where(zero, 1.0, large)
    xs, ys = x * scale, y * scale
    inverse = lax.rsqrt(jnp.where(zero, 1.0, xs * xs + ys * ys))
    half = 0.5 + 0.5 * jnp.abs(xs) * inverse
    root = lax.rsqrt(half)
    big = half * root
    small = 0.5 * jnp.abs(ys) * inverse * root
    ahead = x >= 0.0
    cosine = jnp.where(zero, 1.0, jnp.where(ahead, big, small))
    sine = jnp.where(ahead, small, big)
    sine = jnp.where(zero, 0.0, jnp.where(y < 0.0, -sine, sine))
    at = lambda a, b: (a, b) if a <= b else (b, a)
    pp, qq, pq = matrix[p, p], matrix[q, q], matrix[p, q]
    cc, ss, cs = cosine * cosine, sine * sine, cosine * sine
    new = dict(matrix)
    new[p, p] = cc * pp - 2.0 * cs * pq + ss * qq
    new[q, q] = ss * pp + 2.0 * cs * pq + cc * qq
    new[p, q] = (cc - ss) * pq + cs * (pp - qq)
    for r in range(order):
        if r != p and r != q:
            rp, rq = matrix[at(r, p)], matrix[at(r, q)]
            new[at(r, p)] = cosine * rp - sine * rq
            new[at(r, q)] = sine * rp + cosine * rq
    newv = dict(vectors)
    for r in range(order):
        vp, vq = vectors[r, p], vectors[r, q]
        newv[r, p] = cosine * vp - sine * vq
        newv[r, q] = sine * vp + cosine * vq
    return new, newv


def lowest(matrix, order):
    one = jnp.ones((1, LANES), f32)
    nil = jnp.zeros((1, LANES), f32)
    if order == 1:
        return matrix[0, 0], [one]
    keys = [(a, b) for a in range(order) for b in range(a, order)]
    vkeys = [(a, b) for a in range(order) for b in range(order)]

    def sweep(_, carry):
        m = dict(zip(keys, carry[: len(keys)]))
        v = dict(zip(vkeys, carry[len(keys) :]))
        for p in range(order):
            for q in range(p + 1, order):
                m, v = rotate(m, v, order, p, q)
        return tuple(m[x] for x in keys) + tuple(v[x] for x in vkeys)

    start = tuple(matrix[x] for x in keys) + tuple(one if a == b else nil for a, b in vkeys)
    out = lax.fori_loop(0, SWEEPS, sweep, start)
    m = dict(zip(keys, out[: len(keys)]))
    v = dict(zip(vkeys, out[len(keys) :]))
    theta = m[0, 0]
    weights = [v[r, 0] for r in range(order)]
    for j in range(1, order):
        less = m[j, j] < theta
        theta = jnp.where(less, m[j, j], theta)
        weights = [jnp.where(less, v[r, j], weights[r]) for r in range(order)]
    flip = weights[0] < 0.0
    return theta, [jnp.where(flip, -x, x) for x in weights]


PAIRS = [(a, b) for b in range(ITERS + 1) for a in range(b + 1)]
STATE_ROWS = 4 * len(PAIRS)


def load_state(state_ref, upto):
    state = {}
    for kind in range(4):
        for at, (a, b) in enumerate(PAIRS):
            if b < upto:
                row = kind * len(PAIRS) + at
                state[kind, a, b] = state_ref[row : row + 1, :]
    return state


def store_state(state_ref, state):
    for (kind, a, b), value in state.items():
        row = kind * len(PAIRS) + PAIRS.index((a, b))
        state_ref[row : row + 1, :] = value


def small_problem(count, sums, state):
    n = count - 1
    for a in range(n + 1):
        state[0, a, n] = sums[1 + a : 2 + a, :]
    for a in range(n):
        state[1, a, n] = sums[5 + a : 6 + a, :]
    state[1, n, n] = sums[0:1, :]
    gram = lambda a, b: state[0, min(a, b), max(a, b)]
    mixed = lambda a, b: state[1, min(a, b), max(a, b)]
    one = jnp.ones((1, LANES), f32)
    overlap = [sum(state[2, a, j] * gram(a, n) for a in range(j + 1)) for j in range(n)]
    raw = [-sum(overlap[j] * state[2, a, j] for j in range(a, n)) for a in range(n)] + [one]
    squared = sum(raw[a] * sum(raw[b] * gram(a, b) for b in range(n + 1)) for a in range(n + 1))
    scale = lax.rsqrt(jnp.maximum(squared, 0.0) + epsilon)
    for a in range(n + 1):
        state[2, a, n] = raw[a] * scale
    image = [sum(state[2, b, n] * mixed(a, b) for b in range(n + 1)) for a in range(n + 1)]
    for j in range(n + 1):
        state[3, j, n] = sum(state[2, a, j] * image[a] for a in range(j + 1))
    theta, weights = lowest(
        {(a, b): state[3, a, b] for a in range(count) for b in range(a, count)}, count
    )
    gammas = [sum(weights[j] * state[2, a, j] for j in range(a, count)) for a in range(count)]
    return theta, gammas


def lanes_of(shape):
    return lax.broadcasted_iota(jnp.int32, shape, len(shape) - 1)


def encode(values):
    high = values.astype(bf16).astype(f32)
    rest = values - high
    middle = rest.astype(bf16).astype(f32)
    low = rest - middle
    lane = lanes_of((8, LANES))
    parts = jnp.where(
        lane == 0, high, jnp.where(lane == 1, middle, jnp.where(lane == 2, low, 0.0))
    )
    return jnp.concatenate([parts, jnp.zeros((EXT - 8, LANES), f32)], axis=0).astype(bf16)


def decode(parts):
    return jnp.broadcast_to(jnp.sum(parts[0:8], axis=1, keepdims=True), (8, LANES))


def ext_sum(refs, first):
    total = None
    for ref, count in refs:
        part = ref[0, first : first + EXT, :].astype(f32)
        for b in range(1, count):
            part = part + ref[b, first : first + EXT, :].astype(f32)
        total = part if total is None else total + part
    return total


def scaled_sums(parts, total_count):
    row = lax.broadcasted_iota(jnp.int32, (8, LANES), 0)
    scale = jnp.where(row == 0, 0.5 / total_count, 0.5 / (N_RB * 2 * total_count))
    return decode(parts) * scale


def fold(x):
    return x.reshape(x.shape[0] // 8, 8, x.shape[1]).sum(axis=0)


def apply_kernel(count, total_count, *refs):
    refs = list(refs)
    place = refs.pop(0)
    left, folded = refs.pop(0), refs.pop(0)
    if count == 0:
        guess = [refs.pop(0) for _ in range(4)]
    else:
        diagonal = refs.pop(0)
        state_in = refs.pop(0) if count > 1 else None
        images = [[refs.pop(0) for _ in range(4)] for _ in range(count)]
        vectors = [refs.pop(0) for _ in range(count)]
    out, vector_out = refs.pop(0), refs.pop(0)
    if count > 0:
        state_out = refs.pop(0)
    x_ref, p_ref = refs

    lb, wa = place[0], place[1]
    if count > 0:
        newest = images[-1]
        sums = scaled_sums(
            ext_sum(((newest[0], N_RB), (newest[1], N_RB)), TILE), total_count
        )
        state = load_state(state_in, count - 1) if count > 1 else {}
        theta_row, gamma_rows = small_problem(count, sums, state)
        store_state(state_out, state)
        wide = lambda v: jnp.broadcast_to(v, (HALF, LANES))
        theta = wide(theta_row)
        gammas = [wide(g) for g in gamma_rows]
        deltas = [wide(-theta_row * g) for g in gamma_rows]

    def rows(s):
        return slice(s * HALF, (s + 1) * HALF)

    def cols(s):
        return slice(s * LANES, (s + 1) * LANES)

    n_sums = 1 if count == 0 else 2 * count + 1
    sums_at = tuple(jnp.zeros((8, LANES), f32) for _ in range(n_sums))
    for seg, (base, blocks, other) in enumerate(SEGMENTS):

        def body(b, acc, seg=seg, base=base, other=other):
            acc = list(acc)
            for s in range(S):
                if count == 0:
                    new = guess[seg][b, rows(s), :]
                    olds = []
                else:
                    olds = [v[base + b, rows(s), :].astype(f32) for v in vectors]
                    hs = [h[seg][b, rows(s), :].astype(f32) for h in images]
                    r = gammas[0] * hs[0] + deltas[0] * olds[0]
                    for i in range(1, count):
                        r = r + gammas[i] * hs[i] + deltas[i] * olds[i]
                    d = diagonal[base + b, rows(s), :]
                    new = (r / (jnp.abs(d - theta) + 1.0)).astype(bf16)
                vector_out[base + b, rows(s), :] = new
                if seg < 2:
                    at = pl.multiple_of(b * 2 * HALF + (wa ^ other) * HALF, HALF)
                    x_ref[pl.ds(at, HALF), cols(s)] = new
                    wide_new = new.astype(f32)
                    for i in range(count):
                        acc[i] = acc[i] + fold(olds[i] * wide_new)
                        acc[count + 1 + i] = acc[count + 1 + i] + fold(hs[i] * wide_new)
                    acc[count] = acc[count] + fold(wide_new * wide_new)
            return tuple(acc)

        sums_at = lax.fori_loop(0, blocks, body, sums_at)

    p_ref[...] = jnp.zeros_like(p_ref)

    def product(k, carry):
        y = jnp.dot(left[k], x_ref[...], preferred_element_type=f32).astype(bf16)
        p_ref[...] += jnp.dot(y, folded[k], preferred_element_type=f32)
        return carry

    lax.fori_loop(0, left.shape[0], product, 0)

    quad = jnp.zeros((8, LANES), f32)
    for base, blocks, other in SEGMENTS[2:]:

        def share(j, acc, base=base, other=other):
            rel = jnp.where(j < 4, j, 11 - j)
            at = pl.multiple_of((lb ^ rel) * 2 * HALF + (wa ^ other) * HALF, HALF)
            for s in range(S):
                new = vector_out[base + j, rows(s), :].astype(f32)
                acc = acc + fold(new * p_ref[pl.ds(at, HALF), cols(s)])
            return acc

        quad = lax.fori_loop(0, blocks, share, quad)

    values = [quad] + list(sums_at[: count + 1])
    places = list(range(count + 2))
    values += list(sums_at[count + 1 :])
    places += [5 + i for i in range(count)]
    row = lax.broadcasted_iota(jnp.int32, (8, LANES), 0)
    local = jnp.zeros((8, LANES), f32)
    for at, value in zip(places, values):
        one = jnp.sum(jnp.sum(value, axis=0, keepdims=True), axis=1, keepdims=True)
        local = jnp.where(row == at, jnp.broadcast_to(one, (8, LANES)), local)
    ext = encode(local)

    def write(t, carry):
        at = pl.multiple_of(t * HALF, HALF)
        for s in range(S):
            out[t, rows(s), :] = p_ref[pl.ds(at, HALF), cols(s)].astype(bf16)
        out[t, TILE:, :] = ext
        return carry

    lax.fori_loop(0, out.shape[0], write, 0)


def collect_kernel(parts, image, tile):
    count = parts.shape[0]
    for s in range(S):
        at = slice(s * HALF, (s + 1) * HALF)
        total = parts[0, at, :].astype(f32)
        for t in range(1, count):
            total = total + parts[t, at, :].astype(f32)
        image[at, :] = total
        tile[at, :] = total.astype(bf16)
    tile[TILE:, :] = encode(decode(ext_sum(((parts, count),), TILE)))


def finish_kernel(total_count, *refs):
    count = ITERS + 1
    exts, state_in = refs[0], refs[1]
    images = refs[2 : 2 + count]
    vectors = refs[2 + count : 2 + 2 * count]
    out = refs[-1]
    sums = scaled_sums(ext_sum(((exts, exts.shape[0]),), 0), total_count)
    state = load_state(state_in, count - 1)
    theta_row, gamma_rows = small_problem(count, sums, state)
    wide = lambda v: jnp.broadcast_to(v, (HALF, LANES))
    theta = wide(theta_row)
    gammas = [wide(g) for g in gamma_rows]
    for s in range(S):
        at = slice(s * HALF, (s + 1) * HALF)
        ritz = gammas[0] * vectors[0][0, at, :].astype(f32)
        residual = gammas[0] * images[0][at, :]
        for i in range(1, count):
            ritz = ritz + gammas[i] * vectors[i][0, at, :].astype(f32)
            residual = residual + gammas[i] * images[i][at, :]
        out[0, at, :] = ritz
        out[1, at, :] = residual - theta * ritz


VM = pl.BlockSpec(memory_space=pltpu.VMEM)
SM = pl.BlockSpec(memory_space=pltpu.SMEM)
shaped = jax.ShapeDtypeStruct


def apply(count, total_count, place, left, folded, others):
    outs = [
        shaped((2 * N_LB, TILE + EXT, LANES), bf16),
        shaped((BLOCKS, TILE, LANES), bf16),
    ]
    if count > 0:
        outs.append(shaped((STATE_ROWS, LANES), f32))
    rows_in, rows_out = left.shape[2], left.shape[1]
    width = S * LANES
    return pl.pallas_call(
        functools.partial(apply_kernel, count, total_count),
        out_shape=outs,
        in_specs=[SM] + [VM] * (2 + len(others)),
        out_specs=[VM] * len(outs),
        scratch_shapes=[pltpu.VMEM((rows_in, width), bf16), pltpu.VMEM((rows_out, width), f32)],
        compiler_params=pltpu.CompilerParams(vmem_limit_bytes=56 * 2**20),
        cost_estimate=pl.CostEstimate(
            flops=2 * left.shape[0] * rows_out * width * (rows_in + width),
            bytes_accessed=16 * 2**20,
            transcendentals=0,
        ),
        name=f"apply_{count}",
    )(place, left, folded, *others)


def collect(parts):
    return pl.pallas_call(
        collect_kernel,
        out_shape=[shaped((TILE, LANES), f32), shaped((TILE + EXT, LANES), bf16)],
        in_specs=[VM],
        out_specs=[VM, VM],
        name="collect",
    )(parts)


def finish(total_count, *others):
    return pl.pallas_call(
        functools.partial(finish_kernel, total_count),
        out_shape=shaped((2, TILE, LANES), f32),
        in_specs=[VM] * len(others),
        out_specs=VM,
        name="finish",
    )(*others)


def sent_to_all(x, axis):
    size = lax.axis_size(axis)
    return lax.all_to_all(jnp.broadcast_to(x[None], (size, *x.shape)), axis, 0, 0, tiled=True)


def swapped(x, axis, mask):
    size = lax.axis_size(axis)
    return lax.ppermute(x, axis, [(i, i ^ mask) for i in range(size)])


def gathered(tile):
    block_own = sent_to_all(tile, RB)
    along = tile[None]
    for mask in (1, 2, 7):
        along = jnp.concatenate([along, swapped(along, "lb", mask)], axis=0)
    along_other = swapped(along, "wa", 1)
    block_other = swapped(block_own, "wa", 1)
    return [block_own, block_other, along, along_other]


def dense_operator(operator_blocks, operator_pairs, levels):
    symmetric = 0.5 * (operator_blocks + jnp.swapaxes(operator_blocks, 1, 2))
    indices = jnp.arange(levels, dtype=jnp.int32)
    left_hot = (operator_pairs[:, 0:1] == indices[None, :]).astype(f32)
    right_hot = (operator_pairs[:, 1:2] == indices[None, :]).astype(f32)
    return jnp.einsum("nw,nv,nts->wvts", left_hot, right_hot, symmetric, precision=highest)


def per_device(initial_guess, left_environment, right_environment, operator_blocks, operator_pairs):
    own_rows, physical, window = initial_guess.shape
    levels = right_environment.shape[1]
    local_levels = left_environment.shape[0]
    block_rows = left_environment.shape[1] * left_environment.shape[3]
    contracted = left_environment.shape[4]
    total_count = float(
        own_rows * physical * window * lax.axis_size("lb") * lax.axis_size(RB)
    )
    lb = lax.axis_index("lb")
    rb = lax.axis_index(RB)
    wa = lax.axis_index("wa")
    place = jnp.stack([lb, wa]).astype(jnp.int32)
    left = left_environment.reshape(local_levels, block_rows, contracted)

    own_lines = lax.dynamic_slice_in_dim(left_environment, lb, 1, 1).reshape(
        local_levels, own_rows, contracted
    )
    line = lax.broadcasted_iota(jnp.int32, own_lines.shape, 1)
    column = lax.broadcasted_iota(jnp.int32, own_lines.shape, 2)
    left_diag = jnp.sum(
        jnp.where(column == line + rb * own_rows, own_lines.astype(f32), 0.0), axis=2
    ).astype(bf16)

    guess = lax.dynamic_slice_in_dim(
        jnp.swapaxes(initial_guess, 0, 1), wa * HALF, HALF, 1
    ).reshape(TILE, window)
    ext = jnp.pad(left_diag.reshape(-1, LANES), ((0, EXT - 2), (0, 0)))
    tiles = gathered(jnp.concatenate([guess, ext], axis=0))

    operator = dense_operator(operator_blocks, operator_pairs, levels)
    local_operator = lax.dynamic_slice_in_dim(operator, wa * local_levels, local_levels, 0)
    right_f = right_environment.astype(f32)
    folded = jnp.einsum("kvts,cvb->ksctb", local_operator, right_f, precision=highest)
    folded = folded.reshape(local_levels, physical * window, physical * window).astype(bf16)

    right_diag = jnp.diagonal(right_environment, axis1=0, axis2=2).astype(f32)
    by_level = jnp.einsum(
        "kvs,vb->ksb", jnp.diagonal(operator, axis1=2, axis2=3), right_diag, precision=highest
    )

    def levels_of(own, other):
        halves = [
            t[:, TILE : TILE + 2, :].astype(f32).reshape(-1, local_levels, 2, HALF)
            for t in (own, other)
        ]
        both = jnp.where(
            wa == 0, jnp.concatenate(halves, axis=1), jnp.concatenate(halves[::-1], axis=1)
        )
        first = jnp.where(wa == 0, both[:, :, 0], both[:, :, 1])
        second = jnp.where(wa == 0, both[:, :, 1], both[:, :, 0])
        return jnp.concatenate([first, second], axis=0)

    left_levels = jnp.concatenate(
        [levels_of(tiles[0], tiles[1]), levels_of(tiles[2], tiles[3])], axis=0
    )
    diagonal = jnp.einsum("nki,ksb->nsib", left_levels, by_level, precision=highest)
    diagonal = diagonal.reshape(BLOCKS, TILE, LANES)

    own_images, images, vectors = [], [], []
    state = None
    for count in range(ITERS + 1):
        if count == 0:
            others = tiles
        else:
            others = [diagonal] + ([state] if count > 1 else [])
            others += [t for h in images for t in h] + vectors
        result = apply(count, total_count, place, left, folded, others)
        vectors.append(result[1])
        if count > 0:
            state = result[2]
        arrived = lax.all_to_all(result[0], LB_WA, 0, 0, tiled=True)
        image, tile = collect(arrived)
        own_images.append(image)
        if count < ITERS:
            images.append(gathered(tile))
    exts = sent_to_all(tile[TILE:], RB_WA)
    own = 2 * N_RB
    out = finish(total_count, exts, state, *own_images, *[v[own : own + 1] for v in vectors])
    other = swapped(out, "wa", 1)
    pair = jnp.where(wa == 0, jnp.stack([out, other], 1), jnp.stack([other, out], 1))
    pair = pair.reshape(2, 2, physical, HALF, window)
    pair = jnp.transpose(pair, (0, 1, 3, 2, 4)).reshape(2, own_rows, physical, window)
    return (pair[0], pair[1])


def solution(mesh):
    split = Mesh(
        mesh.devices.reshape(mesh.shape["lb"], 4, 4, mesh.shape["wa"]), ("lb", "rb_0", "rb_1", "wa")
    )
    in_specs = (P(LB_RB, None, None), P("wa", None, RB, None, "lb"), P(), P(), P())
    out_specs = (P(LB_RB, None, None), P(LB_RB, None, None))
    return jax.shard_map(
        per_device, mesh=split, in_specs=in_specs, out_specs=out_specs, check_vma=False
    )
```
